256 devices in a mesh: row: 8 (over x, core), col: 32 (over z, y).
Axes of the slice: x: 4, y: 4, z: 8, core: 2. Of those that a mesh axis runs over, the one named last changes fastest.
Arguments:
- inputs: bfloat16 [2048, 6144], P('col', 'row'), may hold values from -6 to 6
- cotangent: bfloat16 [2048, 6144], P('col', 'row'), may hold values from -6 to 6
- weight_in: bfloat16 [6144, 12288], P('row', 'col'), may hold values from -0.078125 to 0.078125
- moment_in: bfloat16 [6144, 12288], P('row', 'col'), may hold values from -5 to 5
- second_in: bfloat16 [6144, 12288], P('row', 'col'), may hold values from 0.049804688 to 2
- weight_out: bfloat16 [12288, 6144], P('col', 'row'), may hold values from -0.0546875 to 0.0546875
- moment_out: bfloat16 [12288, 6144], P('col', 'row'), may hold values from -5 to 5
- second_out: bfloat16 [12288, 6144], P('col', 'row'), may hold values from 0.049804688 to 2
Outputs:
- input_grad: bfloat16 [2048, 6144], P('col', 'row')
- update_in: bfloat16 [6144, 12288], P('row', 'col')
- code_moment_in: bfloat16 [6144, 12288], P('row', 'col')
- code_second_in: bfloat16 [6144, 12288], P('row', 'col')
- row_scale_in: float32 [2, 6144], P(None, 'row')
- col_scale_in: float32 [2, 12288], P(None, 'col')
- update_out: bfloat16 [12288, 6144], P('col', 'row')
- code_moment_out: bfloat16 [12288, 6144], P('col', 'row')
- code_second_out: bfloat16 [12288, 6144], P('col', 'row')
- row_scale_out: float32 [2, 12288], P(None, 'col')
- col_scale_out: float32 [2, 6144], P(None, 'row')
The draws below stay inside these ranges and needn't reach their ends.
All inputs are finite; a program needn't handle non-finite values. Where the reference program divides by a largest or mean magnitude, that divisor is 1e-20 or more.
Results may differ from the reference program's by a relative error of at most 0.0049.
Values may be sent and summed in bfloat16 or wider, within the bound.
No kernel may reach another device: no remote copies, remote signals or barrier semaphores. Data moves between devices by JAX's collectives and lax.ppermute only.
A program may use at most 64 MiB of HBM per device.

```python
import math
import jax
import jax.numpy as jnp
from jax import lax

D = 6144
FF = 12288
TOKENS = 2048


def block_levels(rng, shape, pieces, least, largest):
    loudness, own = 1.0, jax.random.fold_in(rng, 6)
    for axis_at, parts in pieces:
        steps = jnp.exp(jax.random.uniform(jax.random.fold_in(own, axis_at), (parts,), jnp.float32, least / len(pieces), largest / len(pieces)))
        loudness = loudness * jnp.repeat(steps, shape[axis_at] // parts).reshape([-1 if axis == axis_at else 1 for axis in range(len(shape))])
    return loudness


def noise(key, shape, spread, most, split=(), kind=jnp.bfloat16):
    array = spread * jax.random.normal(key, shape, jnp.float32)
    if split:
        array = array * block_levels(key, shape, split, -0.22, 0.18)
    return jnp.clip(array, -most, most).astype(kind)


def setup_inputs(seed: int = 0) -> dict:
    keys = jax.random.split(jax.random.key(seed), 9)
    return {
        "inputs": noise(keys[0], (TOKENS, D), 1.0, 6.0, ((0, 32), (1, 8))),
        "cotangent": noise(keys[1], (TOKENS, D), 1.0, 6.0, ((0, 32), (1, 8))),
        "weight_in": noise(keys[2], (D, FF), D ** -0.5, 0.078125, ((0, 8), (1, 32))),
        "moment_in": noise(keys[3], (D, FF), 1.0, 5.0, ((0, 8), (1, 32))),
        "second_in": jnp.clip(jnp.exp(math.log(2.0) - 3.6927934 * jax.random.uniform(keys[4], (D, FF), jnp.float32) ** block_levels(keys[4], (D, FF), ((0, 8), (1, 32)), -0.2, 0.2)), 0.049804688, 2.0).astype(jnp.bfloat16),
        "weight_out": noise(keys[5], (FF, D), FF ** -0.5, 0.0546875, ((0, 32), (1, 8))),
        "moment_out": noise(keys[6], (FF, D), 1.0, 5.0, ((0, 32), (1, 8))),
        "second_out": jnp.clip(jnp.exp(math.log(2.0) - 3.6927934 * jax.random.uniform(keys[7], (FF, D), jnp.float32) ** block_levels(keys[7], (FF, D), ((0, 32), (1, 8)), -0.2, 0.2)), 0.049804688, 2.0).astype(jnp.bfloat16),
    }


root_half = 0.7071067811865476
normal_density = 0.3989422804014327
momentum_decay = 0.9
second_decay = 0.95
stable_eps = 1e-08
weight_decay = 0.1

def gelu_parts(preact):
    cumulative = 0.5 * (1.0 + lax.erf(preact * root_half))
    density = jnp.exp(-0.5 * preact * preact) * normal_density
    return (preact * cumulative, cumulative + preact * density)

def optimize(weight, moment, second, gradient, factor):
    scaled = gradient * factor
    moment_new = momentum_decay * moment.astype(jnp.float32) + (1.0 - momentum_decay) * scaled
    second_new = second_decay * second.astype(jnp.float32) + (1.0 - second_decay) * scaled * scaled
    update = moment_new / (jnp.sqrt(second_new) + stable_eps) + weight_decay * weight.astype(jnp.float32)
    row_top = jnp.maximum(jnp.stack([lax.optimization_barrier(jnp.max(jnp.abs(moment_new), axis=1)), lax.optimization_barrier(jnp.max(second_new, axis=1))]), 1.0)
    col_top = jnp.maximum(jnp.stack([lax.optimization_barrier(jnp.max(jnp.abs(moment_new), axis=0)), lax.optimization_barrier(jnp.max(second_new, axis=0))]), 1.0)
    code_moment = moment_new / jnp.minimum(row_top[0][:, None], col_top[0][None, :])
    code_second = second_new / jnp.minimum(row_top[1][:, None], col_top[1][None, :])
    return (update.astype(jnp.bfloat16), code_moment.astype(jnp.bfloat16), code_second.astype(jnp.bfloat16), row_top, col_top)

def reference(inputs, cotangent, weight_in, moment_in, second_in, weight_out, moment_out, second_out):
    preact = jnp.dot(inputs, weight_in, preferred_element_type=jnp.float32)
    hidden_grad = jnp.dot(cotangent, weight_out.T, preferred_element_type=jnp.float32)
    activ_value, slope = gelu_parts(preact)
    hidden = activ_value.astype(jnp.bfloat16)
    delta = (hidden_grad * slope).astype(jnp.bfloat16)
    input_grad = jnp.dot(delta, weight_in.T, preferred_element_type=jnp.float32).astype(jnp.bfloat16)
    grad_in = jnp.dot(inputs.T, delta, preferred_element_type=jnp.float32)
    grad_out = jnp.dot(hidden.T, cotangent, preferred_element_type=jnp.float32)
    total = jnp.sum(grad_in * grad_in) + jnp.sum(grad_out * grad_out)
    factor = 1.0 / jnp.maximum(jnp.sqrt(total / (2.0 * D * FF)), 1.0)
    first = optimize(weight_in, moment_in, second_in, grad_in, factor)
    latter = optimize(weight_out, moment_out, second_out, grad_out, factor)
    return (input_grad, first[0], first[1], first[2], first[3], first[4], latter[0], latter[1], latter[2], latter[3], latter[4])
```

```python
import jax
import jax.numpy as jnp
from jax import lax
from jax.sharding import Mesh
from jax.sharding import PartitionSpec as P


D = 6144
FF = 12288
X, C, Z, Y = "row_0", "row_1", "col_0", "col_1"
COL = (Z, Y)
ROW = (X, C)
FIRST = 24


root_half = 0.7071067811865476
normal_density = 0.3989422804014327
momentum_decay = 0.9
second_decay = 0.95
stable_eps = 1e-08
weight_decay = 0.1


def shift(array, axis, by):
    n = lax.axis_size(axis)
    return lax.ppermute(array, axis, [(i, (i + by) % n) for i in range(n)])


def swap(array, axis, bit):
    n = lax.axis_size(axis)
    return lax.ppermute(array, axis, [(i, i ^ bit) for i in range(n)])


def butterfly(array, axis, combine):
    bit = 1
    while bit < lax.axis_size(axis):
        array = combine(array, swap(array, axis, bit))
        bit *= 2
    return array


def put(whole, piece, *at):
    start = at + (0,) * (whole.ndim - len(at))
    return lax.dynamic_update_slice(whole, piece, start)


def rows(*blocks):
    return jnp.concatenate([b.reshape(-1, b.shape[-1]) for b in blocks], axis=0)


def gather_y(block):
    y = lax.axis_index(Y)
    mine = jnp.zeros((4, *block.shape), block.dtype)
    mine = put(mine, block[None], y)
    came = [shift(block, Y, by) for by in (1, 3, 2)]
    for by, piece in zip((1, 3, 2), came):
        mine = put(mine, piece[None], lax.rem(y + 4 - by, 4))
    return mine


def ring_z(mine):
    first, second = mine[:2], mine[2:]
    up_a, down_a, up_b, down_b = [first], [first], [second], [second]
    for k in range(1, 5):
        up_a.append(shift(up_a[-1], Z, 1))
        if k < 4:
            down_a.append(shift(down_a[-1], Z, -1))
            up_b.append(shift(up_b[-1], Z, 1))
        down_b.append(shift(down_b[-1], Z, -1))
    from_z = lambda k: (down_a[k], down_b[k]) if k <= 3 else (up_a[8 - k], up_b[8 - k])
    opposite = (up_a[4], down_b[4])
    near = [mine, *from_z(1), *from_z(2), *from_z(6), *from_z(7)]
    far = [*from_z(3), *opposite, *from_z(5)]
    return near, far


def gather_z_then_y(block):
    mine = lax.all_to_all(jnp.broadcast_to(block, (8, *block.shape)), Z, 0, 0, tiled=True)
    below, above = shift(mine, Y, 1), shift(mine, Y, -1)
    far_low, far_high = shift(below[:4], Y, 1), shift(above[4:], Y, -1)
    return [mine, above, far_low, far_high, below]


def contract(left, right, left_dim, right_dim):
    return lax.dot_general(
        left, right, (((left_dim,), (right_dim,)), ((), ())), preferred_element_type=jnp.float32
    )


def activate(preact, hidden_grad):
    cumulative = 0.5 * (1.0 + lax.erf(preact * root_half))
    density = jnp.exp(-0.5 * preact * preact) * normal_density
    hidden = (preact * cumulative).astype(jnp.bfloat16)
    delta = (hidden_grad * (cumulative + preact * density)).astype(jnp.bfloat16)
    return (hidden, delta)


def summed(blocks, axis):
    came = lax.all_to_all(blocks.astype(jnp.bfloat16), axis, 0, 0, tiled=True)
    return jnp.sum(came.astype(jnp.float32), axis=0)


def hidden_and_delta(tokens, weight_in, weight_out):
    width, units = weight_in.shape
    n = tokens.shape[0]
    preact = jnp.dot(tokens[:, :width], weight_in, preferred_element_type=jnp.float32)
    grad = contract(tokens[:, width:], weight_out, 1, 1)
    part = jnp.concatenate([preact.astype(jnp.bfloat16), grad.astype(jnp.bfloat16)], axis=1)
    stacked = summed(part.reshape(4, n // 4, 2 * units), X)
    hidden, delta = activate(stacked[:, :units], stacked[:, units:])
    own = jnp.concatenate([hidden, delta], axis=1)
    x = lax.axis_index(X)
    both = put(jnp.zeros((4, *own.shape), own.dtype), own[None], x)
    came = [shift(own, X, by) for by in (1, 3, 2)]
    for by, piece in zip((1, 3, 2), came):
        both = put(both, piece[None], lax.rem(x + 4 - by, 4))
    both = both.reshape(n, 2 * units)
    return (both[:, :units], both[:, units:])


def moments(weight, moment, second, gradient, factor):
    scaled = gradient * factor
    moment_new = momentum_decay * moment.astype(jnp.float32) + (1.0 - momentum_decay) * scaled
    second_new = second_decay * second.astype(jnp.float32) + (1.0 - second_decay) * scaled * scaled
    update = moment_new / (jnp.sqrt(second_new) + stable_eps) + weight_decay * weight.astype(
        jnp.float32
    )
    row_local = jnp.stack([jnp.max(jnp.abs(moment_new), axis=1), jnp.max(second_new, axis=1)])
    col_local = jnp.stack([jnp.max(jnp.abs(moment_new), axis=0), jnp.max(second_new, axis=0)])
    return (update.astype(jnp.bfloat16), moment_new, second_new, row_local, col_local)


def encode(moment_new, second_new, row_top, col_top):
    row_top = jnp.maximum(row_top, 1.0)
    col_top = jnp.maximum(col_top, 1.0)
    code_moment = moment_new / jnp.minimum(row_top[0][:, None], col_top[0][None, :])
    code_second = second_new / jnp.minimum(row_top[1][:, None], col_top[1][None, :])
    return (code_moment.astype(jnp.bfloat16), code_second.astype(jnp.bfloat16), row_top, col_top)


def program(inputs, cotangent, weight_in, moment_in, second_in, weight_out, moment_out, second_out):
    width = inputs.shape[1]
    core = lax.axis_index(C)
    halves = jnp.concatenate([inputs, cotangent], axis=1).reshape(2, 32, 2 * width)
    own = lax.dynamic_index_in_dim(halves, core, 0, keepdims=False)
    came = swap(lax.dynamic_index_in_dim(halves, 1 - core, 0, keepdims=False), C, 1)
    block = jnp.concatenate(
        [own[:, :width], came[:, :width], own[:, width:], came[:, width:]], axis=1
    )
    wide = 2 * width
    both_in = jnp.concatenate([weight_in, swap(weight_in, C, 1)], axis=0)
    both_out = jnp.concatenate([weight_out, swap(weight_out, C, 1)], axis=1)

    mine = gather_y(block[:FIRST])
    rest = gather_z_then_y(block[FIRST:])
    near, far = ring_z(mine)
    tokens_a = rows(*rest, *near)
    tokens_b = rows(*far)
    hidden_a, delta_a = hidden_and_delta(tokens_a, both_in, both_out)
    hidden_b, delta_b = hidden_and_delta(tokens_b, both_in, both_out)

    def gradients(low, high):
        grad_in = contract(tokens_a[:, low:high], delta_a, 0, 0)
        grad_in += contract(tokens_b[:, low:high], delta_b, 0, 0)
        grad_out = contract(hidden_a, tokens_a[:, wide + low : wide + high], 0, 0)
        grad_out += contract(hidden_b, tokens_b[:, wide + low : wide + high], 0, 0)
        return (grad_in, grad_out)

    y, z = lax.axis_index(Y), lax.axis_index(Z)
    back_a = contract(delta_a, both_in, 1, 1).astype(jnp.bfloat16)
    back_b = contract(delta_b, both_in, 1, 1).astype(jnp.bfloat16)
    n_rest = 8 * 4 * (32 - FIRST)
    back_rest = back_a[:n_rest].reshape(4, 8, 32 - FIRST, wide)
    back_rest = jnp.concatenate([back_rest, back_rest], axis=0)
    back_rest = lax.dynamic_slice_in_dim(back_rest, lax.rem(4 - y, 4), 4, axis=0)
    back_near = back_a[n_rest:].reshape(5, 4, FIRST, wide)
    back_far = back_b.reshape(3, 4, FIRST, wide)
    back_a = jnp.concatenate(
        [
            back_rest.reshape(4, -1, wide),
            back_near.transpose(1, 0, 2, 3).reshape(4, -1, wide),
        ],
        axis=1,
    )
    back_a = summed(back_a, Y)
    back_b = back_far.transpose(1, 0, 2, 3).reshape(4, -1, wide)
    back_b = summed(back_b, Y)
    n_rest = 8 * (32 - FIRST)
    back_rest = back_a[:n_rest].reshape(8, 32 - FIRST, wide)
    back_near = back_a[n_rest:].reshape(5, FIRST, wide)
    back_far = back_b.reshape(3, FIRST, wide)
    ring = jnp.concatenate([back_near[:3], back_far, back_near[3:]], axis=0)
    ring = lax.dynamic_slice_in_dim(
        jnp.concatenate([ring, ring], axis=0), lax.rem(8 - z, 8), 8, axis=0
    )
    back = jnp.concatenate([ring, back_rest], axis=1)
    back = summed(back, Z)
    came = swap(back[:, width:], C, 1)
    first = core == 0
    low = jnp.where(first, back[:, :width], came)
    high = jnp.where(first, came, back[:, :width])
    input_grad = jnp.concatenate([low, high], axis=0).astype(jnp.bfloat16)

    other_in, other_out = gradients(width, wide)
    other_in, other_out = swap(other_in, C, 1), swap(other_out, C, 1)
    grad_in, grad_out = gradients(0, width)
    grad_in += other_in
    grad_out += other_out
    local_total = jnp.sum(grad_in * grad_in) + jnp.sum(grad_out * grad_out)
    total = jnp.full((8, 128), local_total)
    for axis in (C, X, Z, Y):
        total = butterfly(total, axis, jnp.add)
    factor = 1.0 / jnp.maximum(jnp.sqrt(total[0, 0] / (2.0 * D * FF)), 1.0)

    update_in, moment_new_in, second_new_in, rows_in, cols_in = moments(
        weight_in, moment_in, second_in, grad_in, factor
    )
    update_out, moment_new_out, second_new_out, rows_out, cols_out = moments(
        weight_out, moment_out, second_out, grad_out, factor
    )
    over_col = jnp.concatenate([rows_in, cols_out], axis=0)
    over_row = jnp.concatenate([cols_in, rows_out], axis=0)
    for axis in (C, X):
        over_row = butterfly(over_row, axis, jnp.maximum)
    for axis in (Y, Z):
        over_col = butterfly(over_col, axis, jnp.maximum)
    code_moment_in, code_second_in, row_scale_in, col_scale_in = encode(
        moment_new_in, second_new_in, over_col[:2], over_row[:2]
    )
    code_moment_out, code_second_out, row_scale_out, col_scale_out = encode(
        moment_new_out, second_new_out, over_row[2:], over_col[2:]
    )
    return (
        input_grad,
        update_in,
        code_moment_in,
        code_second_in,
        row_scale_in,
        col_scale_in,
        update_out,
        code_moment_out,
        code_second_out,
        row_scale_out,
        col_scale_out,
    )


def solution(mesh):
    split = Mesh(mesh.devices.reshape(4, 2, 8, 4), (X, C, Z, Y))
    placed = (
        P(COL, ROW),
        P(COL, ROW),
        P(ROW, COL),
        P(ROW, COL),
        P(ROW, COL),
        P(COL, ROW),
        P(COL, ROW),
        P(COL, ROW),
    )
    return jax.shard_map(
        program,
        mesh=split,
        in_specs=placed,
        out_specs=(
            P(COL, ROW),
            P(ROW, COL),
            P(ROW, COL),
            P(ROW, COL),
            P(None, ROW),
            P(None, COL),
            P(COL, ROW),
            P(COL, ROW),
            P(COL, ROW),
            P(None, COL),
            P(None, ROW),
        ),
        check_vma=False,
    )
```

```python
import functools

import jax
import jax.numpy as jnp
from jax import lax
from jax.experimental import pallas as pl
from jax.experimental.pallas import tpu as pltpu
from jax.sharding import Mesh
from jax.sharding import PartitionSpec as P


D = 6144
FF = 12288
X, C, Z, Y = "row_0", "row_1", "col_0", "col_1"
COL = (Z, Y)
ROW = (X, C)
FIRST = 24


root_half = 0.7071067811865476
normal_density = 0.3989422804014327
momentum_decay = 0.9
second_decay = 0.95
stable_eps = 1e-08
weight_decay = 0.1


def shift(array, axis, by):
    n = lax.axis_size(axis)
    return lax.ppermute(array, axis, [(i, (i + by) % n) for i in range(n)])


def swap(array, axis, bit):
    n = lax.axis_size(axis)
    return lax.ppermute(array, axis, [(i, i ^ bit) for i in range(n)])


def butterfly(array, axis, combine):
    bit = 1
    while bit < lax.axis_size(axis):
        array = combine(array, swap(array, axis, bit))
        bit *= 2
    return array


def put(whole, piece, *at):
    start = at + (0,) * (whole.ndim - len(at))
    return lax.dynamic_update_slice(whole, piece, start)


def pack_kernel(places, y_ref, *refs):
    blocks, (in_ref, out_ref, x_ref, part_ref) = refs[: len(places)], refs[len(places) :]
    y = y_ref[0]
    for block, (by, per, at) in zip(blocks, places):
        n = block.shape[0]
        if by is None:
            x_ref[at : at + n, :] = block[...]
        else:
            start = pl.multiple_of(lax.rem(y + by, 4) * per + at, 32)
            x_ref[pl.ds(start, n), :] = block[...]
    wide, units = in_ref.shape
    n = x_ref.shape[0]
    tile = n // 2
    for at in range(0, n, tile):
        part_ref[at : at + tile, :units] = jnp.dot(
            x_ref[at : at + tile, :wide], in_ref[...], preferred_element_type=jnp.float32
        ).astype(jnp.bfloat16)
        part_ref[at : at + tile, units:] = contract(
            x_ref[at : at + tile, wide:], out_ref[...], 1, 1
        ).astype(jnp.bfloat16)


def pack_and_project(blocks, places, weight_in, weight_out):
    blocks = [b.reshape(-1, b.shape[-1]) for b in blocks]
    wide, units = weight_in.shape
    n = sum(b.shape[0] for b in blocks)
    whole = pl.BlockSpec(memory_space=pltpu.VMEM)
    return pl.pallas_call(
        functools.partial(pack_kernel, places),
        out_shape=(
            jax.ShapeDtypeStruct((n, 2 * wide), jnp.bfloat16),
            jax.ShapeDtypeStruct((n, 2 * units), jnp.bfloat16),
        ),
        in_specs=[pl.BlockSpec(memory_space=pltpu.SMEM)] + [whole] * (len(blocks) + 2),
        out_specs=(whole, whole),
        compiler_params=pltpu.CompilerParams(vmem_limit_bytes=16 * 1024 * 1024),
        cost_estimate=pl.CostEstimate(
            flops=4 * n * wide * units, bytes_accessed=8 * n * wide, transcendentals=0
        ),
    )(lax.axis_index(Y).reshape(1), *blocks, weight_in, weight_out)


def from_all(block, axis):
    n = lax.axis_size(axis)
    return lax.all_to_all(jnp.broadcast_to(block, (n, *block.shape)), axis, 0, 0, tiled=True)


def roll_kernel(n_rest, z_ref, came_ref, out_ref):
    came = came_ref[...]
    z = z_ref[0]
    out_ref[:, FIRST:, :] = came[:n_rest].reshape(8, 32 - FIRST, -1)
    for i, by in enumerate((0, 1, 2, 6, 7, 3, 4, 5)):
        at = n_rest + i * FIRST
        out_ref[lax.rem(z + by, 8), :FIRST, :] = came[at : at + FIRST]


def roll(came):
    whole = pl.BlockSpec(memory_space=pltpu.VMEM)
    return pl.pallas_call(
        functools.partial(roll_kernel, 8 * (32 - FIRST)),
        out_shape=jax.ShapeDtypeStruct((8, 32, came.shape[1]), came.dtype),
        in_specs=[pl.BlockSpec(memory_space=pltpu.SMEM), whole],
        out_specs=whole,
        compiler_params=pltpu.CompilerParams(vmem_limit_bytes=4 * 1024 * 1024),
        cost_estimate=pl.CostEstimate(flops=came.size, bytes_accessed=6 * came.size, transcendentals=0),
    )(lax.axis_index(Z).reshape(1), came)


def gather_y(block):
    y = lax.axis_index(Y)
    mine = jnp.zeros((4, *block.shape), block.dtype)
    mine = put(mine, block[None], y)
    came = [shift(block, Y, by) for by in (1, 3, 2)]
    for by, piece in zip((1, 3, 2), came):
        mine = put(mine, piece[None], lax.rem(y + 4 - by, 4))
    return mine


def ring_z(mine):
    first, second = mine[:2], mine[2:]
    up_a, down_a, up_b, down_b = [first], [first], [second], [second]
    for k in range(1, 5):
        up_a.append(shift(up_a[-1], Z, 1))
        if k < 4:
            down_a.append(shift(down_a[-1], Z, -1))
            up_b.append(shift(up_b[-1], Z, 1))
        down_b.append(shift(down_b[-1], Z, -1))
    from_z = lambda k: (down_a[k], down_b[k]) if k <= 3 else (up_a[8 - k], up_b[8 - k])
    opposite = (up_a[4], down_b[4])
    near = [mine, *from_z(1), *from_z(2), *from_z(6), *from_z(7)]
    far = [*from_z(3), *opposite, *from_z(5)]
    return near, far


def gather_z_then_y(block):
    mine = from_all(block, Z)
    below, above = shift(mine, Y, 1), shift(mine, Y, -1)
    far_low, far_high = shift(below[:4], Y, 1), shift(above[4:], Y, -1)
    return [mine, above, far_low, far_high, below]


def contract(left, right, left_dim, right_dim):
    return lax.dot_general(
        left, right, (((left_dim,), (right_dim,)), ((), ())), preferred_element_type=jnp.float32
    )


def activate(preact, hidden_grad):
    cumulative = 0.5 * (1.0 + lax.erf(preact * root_half))
    density = jnp.exp(-0.5 * preact * preact) * normal_density
    hidden = (preact * cumulative).astype(jnp.bfloat16)
    delta = (hidden_grad * (cumulative + preact * density)).astype(jnp.bfloat16)
    return (hidden, delta)


def summed(blocks, axis):
    came = lax.all_to_all(blocks.astype(jnp.bfloat16), axis, 0, 0, tiled=True)
    return jnp.sum(came.astype(jnp.float32), axis=0)


def own_hidden_and_delta(part):
    n, units = part.shape[0], part.shape[1] // 2
    stacked = summed(part.reshape(4, n // 4, 2 * units), X)
    hidden, delta = activate(stacked[:, :units], stacked[:, units:])
    return jnp.concatenate([hidden, delta], axis=1)


def moments(weight, moment, second, gradient, factor):
    scaled = gradient * factor
    moment_new = momentum_decay * moment.astype(jnp.float32) + (1.0 - momentum_decay) * scaled
    second_new = second_decay * second.astype(jnp.float32) + (1.0 - second_decay) * scaled * scaled
    update = moment_new / (jnp.sqrt(second_new) + stable_eps) + weight_decay * weight.astype(
        jnp.float32
    )
    row_local = jnp.stack([jnp.max(jnp.abs(moment_new), axis=1), jnp.max(second_new, axis=1)])
    col_local = jnp.stack([jnp.max(jnp.abs(moment_new), axis=0), jnp.max(second_new, axis=0)])
    return (update.astype(jnp.bfloat16), moment_new, second_new, row_local, col_local)


def encode(moment_new, second_new, row_top, col_top):
    row_top = jnp.maximum(row_top, 1.0)
    col_top = jnp.maximum(col_top, 1.0)
    code_moment = moment_new / jnp.minimum(row_top[0][:, None], col_top[0][None, :])
    code_second = second_new / jnp.minimum(row_top[1][:, None], col_top[1][None, :])
    return (code_moment.astype(jnp.bfloat16), code_second.astype(jnp.bfloat16), row_top, col_top)


def program(inputs, cotangent, weight_in, moment_in, second_in, weight_out, moment_out, second_out):
    width = inputs.shape[1]
    core = lax.axis_index(C)
    halves = jnp.concatenate([inputs, cotangent], axis=1).reshape(2, 32, 2 * width)
    own = lax.dynamic_index_in_dim(halves, core, 0, keepdims=False)
    came = swap(lax.dynamic_index_in_dim(halves, 1 - core, 0, keepdims=False), C, 1)
    block = jnp.concatenate(
        [own[:, :width], came[:, :width], own[:, width:], came[:, width:]], axis=1
    )
    wide = 2 * width
    both_in = jnp.concatenate([weight_in, swap(weight_in, C, 1)], axis=0)
    both_out = jnp.concatenate([weight_out, swap(weight_out, C, 1)], axis=1)

    mine = gather_y(block[:FIRST])
    rest = gather_z_then_y(block[FIRST:])
    near, far = ring_z(mine)
    per = 8 * (32 - FIRST)
    at, near_at, far_at = 4 * per, [], []
    for piece in near:
        near_at.append((None, 0, at))
        at += piece.size // piece.shape[-1]
    at = 0
    for piece in far:
        far_at.append((None, 0, at))
        at += piece.size // piece.shape[-1]
    rest_at = [(0, per, 0), (1, per, 0), (2, per, 0), (2, per, per // 2), (3, per, 0)]
    tokens_a, part_a = pack_and_project([*rest, *near], tuple(rest_at + near_at), both_in, both_out)
    tokens_b, part_b = pack_and_project(far, tuple(far_at), both_in, both_out)
    own_a, own_b = own_hidden_and_delta(part_a), own_hidden_and_delta(part_b)
    both = from_all(jnp.concatenate([own_a, own_b], axis=0), X)
    n_a, units = own_a.shape[0], weight_in.shape[1]
    both_a = both[:, :n_a].reshape(4 * n_a, 2 * units)
    both_b = both[:, n_a:].reshape(-1, 2 * units)
    hidden_a, delta_a = both_a[:, :units], both_a[:, units:]
    hidden_b, delta_b = both_b[:, :units], both_b[:, units:]

    def gradients(low, high):
        grad_in = contract(tokens_a[:, low:high], delta_a, 0, 0)
        grad_in += contract(tokens_b[:, low:high], delta_b, 0, 0)
        grad_out = contract(hidden_a, tokens_a[:, wide + low : wide + high], 0, 0)
        grad_out += contract(hidden_b, tokens_b[:, wide + low : wide + high], 0, 0)
        return (grad_in, grad_out)

    back_a = contract(delta_a, both_in, 1, 1).astype(jnp.bfloat16)
    back_b = contract(delta_b, both_in, 1, 1).astype(jnp.bfloat16)
    n_rest = 8 * 4 * (32 - FIRST)
    back_rest = back_a[:n_rest].reshape(4, -1, wide)
    back_near = back_a[n_rest:].reshape(5, 4, FIRST, wide)
    back_far = back_b.reshape(3, 4, FIRST, wide)
    back_near = back_near.transpose(1, 0, 2, 3).reshape(4, -1, wide)
    back_far = back_far.transpose(1, 0, 2, 3).reshape(4, -1, wide)
    back = jnp.concatenate([back_rest, back_near, back_far], axis=1)
    back = summed(back, Y).astype(jnp.bfloat16)
    other_in, other_out = gradients(width, wide)
    other_in, other_out = swap(other_in, C, 1), swap(other_out, C, 1)
    grad_in, grad_out = gradients(0, width)
    grad_in += other_in
    grad_out += other_out
    local_total = jnp.sum(grad_in * grad_in) + jnp.sum(grad_out * grad_out)
    total = jnp.full((8, 128), local_total)
    for axis in (C, X):
        total = butterfly(total, axis, jnp.add)
    total = jnp.sum(from_all(total[:1], COL), axis=0)
    factor = 1.0 / jnp.maximum(jnp.sqrt(total[0, 0] / (2.0 * D * FF)), 1.0)

    back = roll(back)
    back = summed(back, Z)
    came = swap(back[:, width:], C, 1)
    first = core == 0
    low = jnp.where(first, back[:, :width], came)
    high = jnp.where(first, came, back[:, :width])
    input_grad = jnp.concatenate([low, high], axis=0).astype(jnp.bfloat16)

    update_in, moment_new_in, second_new_in, rows_in, cols_in = moments(
        weight_in, moment_in, second_in, grad_in, factor
    )
    update_out, moment_new_out, second_new_out, rows_out, cols_out = moments(
        weight_out, moment_out, second_out, grad_out, factor
    )
    over_col = jnp.concatenate([rows_in, cols_out], axis=0)
    over_row = jnp.concatenate([cols_in, rows_out], axis=0)
    for axis in (C, X):
        over_row = butterfly(over_row, axis, jnp.maximum)
    over_col = butterfly(over_col, Y, jnp.maximum)
    over_col = from_all(over_col.reshape(1, -1), Z)
    over_col = jnp.max(over_col, axis=0).reshape(4, -1)
    code_moment_in, code_second_in, row_scale_in, col_scale_in = encode(
        moment_new_in, second_new_in, over_col[:2], over_row[:2]
    )
    code_moment_out, code_second_out, row_scale_out, col_scale_out = encode(
        moment_new_out, second_new_out, over_row[2:], over_col[2:]
    )
    return (
        input_grad,
        update_in,
        code_moment_in,
        code_second_in,
        row_scale_in,
        col_scale_in,
        update_out,
        code_moment_out,
        code_second_out,
        row_scale_out,
        col_scale_out,
    )


def solution(mesh):
    split = Mesh(mesh.devices.reshape(4, 2, 8, 4), (X, C, Z, Y))
    placed = (
        P(COL, ROW),
        P(COL, ROW),
        P(ROW, COL),
        P(ROW, COL),
        P(ROW, COL),
        P(COL, ROW),
        P(COL, ROW),
        P(COL, ROW),
    )
    return jax.shard_map(
        program,
        mesh=split,
        in_specs=placed,
        out_specs=(
            P(COL, ROW),
            P(ROW, COL),
            P(ROW, COL),
            P(ROW, COL),
            P(None, ROW),
            P(None, COL),
            P(COL, ROW),
            P(COL, ROW),
            P(COL, ROW),
            P(None, COL),
            P(None, ROW),
        ),
        check_vma=False,
    )
```
